32 devices in a mesh: col: 4 (over y, core), row: 8 (over z, x).
Axes of the slice: x: 2, y: 2, z: 4, core: 2. Of those that a mesh axis runs over, the one named last changes fastest.
Arguments:
- column_table: float32 [32768, 512], P('row', 'col'), may hold values from -3 to 3
- bag_rows: int32 [256, 32], P('row'), may hold values from 0 to 32767
Outputs:
- row_table: float32 [8, 4096, 512], P(None, ('col', 'row'))
- pooled: float32 [256, 512], P('row', 'col')
The draws below stay inside these ranges and needn't reach their ends.
Inputs may be any that keep to these rules, and one draw needn't show every extreme that they name: `bag_rows`: row indices of the table; a few rows are named far more often than the rest.
All inputs are finite; a program needn't handle non-finite values.
Results may differ from the reference program's by a relative error of at most 0.000078.
Values sent between devices are 32-bit elements; how exact they have to be, the bound alone decides.
A program may use at most 64 MiB of HBM per device.

```python
import math
import jax
import jax.numpy as jnp
import numpy as np

E = 512
BAG_LEN = 32
ROWS = 32768
GROUPS = 8
BLOCK = 4096
BAGS = 256


def plant(drawn, own_key, low, top_value):
    place = [jax.random.randint(jax.random.fold_in(own_key, axis), (), 0, length) for axis, length in enumerate(drawn.shape)]
    longest = drawn.shape.index(max(drawn.shape))
    next_to = place[:longest] + [(place[longest] + 1) % drawn.shape[longest]] + place[longest + 1:]
    return drawn.at[tuple(place)].set(low).at[tuple(next_to)].set(top_value)


def steps_of(rng, shape, pieces, low, largest):
    gain = 1.0
    for position, shards_of in pieces:
        draws = jax.random.uniform(jax.random.fold_in(jax.random.fold_in(rng, 6), position), (shards_of,), jnp.float32, low / len(pieces), largest / len(pieces))
        gain = gain * jnp.repeat(jnp.exp(draws), shape[position] // shards_of).reshape((-1,) + (1,) * (len(shape) - 1 - position))
    return gain


def cumulative_ranks(count, lean):
    weights = [(1 << 20) // math.isqrt(grade ** lean) + 1 for grade in range(1, count + 1)]
    spread = 1 + sum(weights) // (1 << 30)
    return np.cumsum(np.array([max(1, weight // spread) for weight in weights]))


def ranked(own_key, dims, count, skew):
    table = cumulative_ranks(count, skew)
    lot = jax.random.randint(jax.random.fold_in(own_key, 1), dims, 0, int(table[count - 1]))
    standing = jnp.searchsorted(jnp.asarray(table, jnp.int32), lot, side="right")
    return jax.random.permutation(jax.random.fold_in(own_key, 2), count)[standing].astype(jnp.int32)


def bell_draw(rng, dims, scale, most, cuts=(), held_as=jnp.bfloat16):
    factor_of = steps_of(rng, dims, cuts, -0.22, 0.18) if cuts else 1.0
    values = jax.random.normal(rng, dims, jnp.float32) * scale * factor_of
    return jnp.minimum(jnp.maximum(values, -most), most).astype(held_as)


def setup_inputs(seed: int = 0) -> dict:
    key_list = jax.random.split(jax.random.key(seed), 3)
    column_table = bell_draw(key_list[0], (ROWS, E), 0.2, 3.0, ((0, 8), (1, 4)), jnp.float32)
    bag_rows = plant(ranked(key_list[1], (BAGS, BAG_LEN), ROWS, 2), jax.random.fold_in(key_list[1], 3), 0, ROWS - 1).astype(jnp.int32)
    return {"column_table": column_table, "bag_rows": bag_rows}


def reference(column_table, bag_rows):
    row_table = column_table.reshape(GROUPS, BLOCK, E)
    picked = jnp.take(column_table, bag_rows.reshape(-1), axis=0).reshape(BAGS, BAG_LEN, E)
    pooled = jnp.sum(picked.astype(jnp.float32), axis=1)
    return row_table, pooled
```

```python
import functools
import math

import jax
import jax.numpy as jnp
from jax import lax
from jax.experimental import pallas as pl
from jax.experimental.pallas import tpu as pltpu
from jax.sharding import PartitionSpec as P

MESH = pl.DeviceIdType.MESH
LANES = 128
SUBLANES = 8


def pooling(positions, table_rows):
    row_count = table_rows.shape[0]
    bag_count = positions.shape[0]
    block_rows = math.gcd(row_count, 512)
    turns = row_count // block_rows
    running = jnp.zeros((bag_count, table_rows.shape[1]), jnp.float32)
    tile_ids = jnp.arange(block_rows, dtype=jnp.int32)

    def advance(turn, carried):
        offset = turn * block_rows
        within = positions - offset
        matches = within[:, :, None] == tile_ids[None, None, :]
        counts = jnp.sum(matches.astype(jnp.float32), axis=1)
        table_block = lax.dynamic_slice_in_dim(table_rows, offset, block_rows, 0)
        return carried + jnp.dot(
            counts, table_block, precision=lax.Precision.HIGHEST, preferred_element_type=jnp.float32
        )

    return lax.fori_loop(0, turns, advance, running)


def general(column_table, bag_rows):
    row_groups = lax.axis_size("row")
    col_groups = lax.axis_size("col")
    block_len, col_width = column_table.shape
    full_width = col_width * col_groups
    span = block_len // (col_groups * row_groups)
    row_index = lax.axis_index("row")
    every_bag = lax.all_gather(bag_rows, "row", axis=0, tiled=True)
    sectioned = column_table.reshape(col_groups, row_groups, span, col_width)
    moved = lax.all_to_all(
        lax.all_to_all(sectioned, "col", split_axis=0, concat_axis=3, tiled=True),
        "row",
        split_axis=1,
        concat_axis=0,
        tiled=True,
    )
    row_table = moved.reshape(row_groups, span, full_width)
    first_row = row_index * block_len
    shifted = every_bag - first_row
    inside = (shifted >= 0) & (shifted < block_len)
    positions = jnp.where(inside, shifted, -1)
    pooled = lax.psum_scatter(
        pooling(positions, column_table), "row", scatter_dimension=0, tiled=True
    )
    return (row_table, pooled)


def flipped(index, mask, count):
    result, bit = 0, 1
    while bit < count:
        total = lax.div(index, bit) + (mask // bit if isinstance(mask, int) else lax.div(mask, bit))
        result = result + lax.rem(total, 2) * bit
        bit *= 2
    return result


def orders(rows, cols):
    step, half, across = rows // 4, rows // 2, cols // 2
    masks = [(mr, mc) for mr in range(rows) for mc in range(cols)]
    spread = lambda m: -((m[0] % step > 0) + (m[1] >= across))
    first = [(3 * step, 0)]
    second = [(3 * step + 1, 0), (3 * step + 1, 1), (3 * step, across), (3 * step, across + 1)]
    last = (3 * step, 1)
    near = [m for m in masks if m[0] < step and m != (0, 0)]
    beside = [m for m in masks if step <= m[0] < half]
    two = sorted((m for m in masks if half <= m[0] < 3 * step), key=spread)
    three = sorted((m for m in masks if m[0] >= 3 * step), key=spread)
    left = [m for m in three if m not in first + second + [last]]
    inner = two + left + [last]
    outer = two + three
    return first, second, inner, outer, near, beside


def kernel(
    row_groups, col_groups,
    table_ref, bags_ref, out_ref, pooled_ref,
    table_v, bags_v, gathered, counts, partial, arrived, halves, crossed,
    load_sem, bag_sem, own_sem, pair_sem, all_sem, send_sem, recv_sem,
    bag_send, bag_recv, sum_send, sum_recv, cross_send, cross_recv,
):
    rows, cols = row_groups, col_groups
    r, c = lax.axis_index("row"), lax.axis_index("col")
    block_len, width = table_ref.shape
    span = block_len // (rows * cols)
    own_bags, bag_len = bags_ref.shape
    per_vreg = LANES // bag_len
    half, step = rows // 2, rows // 4
    plane = lax.div(r, step)
    inner = (plane == 1) | (plane == 2)
    outer = (plane == 0) | (plane == 3)

    first, second, inner_order, outer_order, near, beside = orders(rows, cols)
    masks = [(mr, mc) for mr in range(rows) for mc in range(cols)]
    others = [m for m in masks if m != (0, 0)]
    meets = first + [(3 * step, 1), (1, 0), (0, cols // 2)]

    def peer(mask):
        return flipped(r, mask[0], rows), flipped(c, mask[1], cols)

    def at(mask):
        pr, pc = peer(mask)
        return pl.ds((pc * rows + pr) * span, span)

    def signal(sem, mask):
        pr, pc = peer(mask)
        pl.semaphore_signal(sem, inc=1, device_id=(pc, pr), device_id_type=MESH)

    def load(mask):
        return pltpu.make_async_copy(
            table_ref.at[at(mask), :], table_v.at[at(mask), :], load_sem.at[mask[0] * cols + mask[1]]
        )

    def bulk(mask):
        pr, pc = peer(mask)
        return pltpu.make_async_remote_copy(
            src_ref=table_v.at[at(mask), :], dst_ref=out_ref.at[r, c],
            send_sem=send_sem, recv_sem=recv_sem,
            device_id=(pc, pr), device_id_type=MESH,
        )

    def send(chosen):
        for mask in chosen:
            bulk(mask).start()

    bag_load = pltpu.make_async_copy(bags_ref, bags_v, bag_sem)
    bag_load.start()
    barrier = pltpu.get_barrier_semaphore()

    @pl.when(inner)
    def _():
        for mask in meets:
            signal(barrier, mask)

    for mask in first + second:
        load(mask).start()

    @pl.when(inner)
    def _():
        for mask in others:
            if mask[0] // step in (1, 2):
                signal(barrier, mask)

    @pl.when(outer)
    def _():
        for mask in others:
            if mask[0] // step in (0, 3):
                signal(barrier, mask)

    for mask in inner_order + near + beside + [(0, 0)]:
        load(mask).start()
    own = pltpu.make_async_copy(table_ref.at[at((0, 0)), :], out_ref.at[r, c], own_sem)
    own.start()

    def bag(mask):
        pr, _ = peer((mask, 0))
        return pltpu.make_async_remote_copy(
            src_ref=gathered.at[r], dst_ref=gathered.at[r],
            send_sem=bag_send.at[mask], recv_sem=bag_recv.at[mask],
            device_id=(c, pr), device_id_type=MESH,
        )

    def pair(mask, source):
        pr, _ = peer((step, 0))
        rows_of = pl.ds(lax.div(flipped(r, source, rows), step) * step, step)
        return pltpu.make_async_remote_copy(
            src_ref=gathered.at[rows_of], dst_ref=gathered.at[rows_of],
            send_sem=bag_send.at[mask], recv_sem=bag_recv.at[mask],
            device_id=(c, pr), device_id_type=MESH,
        )

    bag_load.wait()
    gathered[r] = jnp.concatenate(
        [bags_v[pl.ds(q, SUBLANES, stride=per_vreg), :] for q in range(per_vreg)], axis=1
    )
    for mask in first + second:
        load(mask).wait()

    @pl.when(inner)
    def _():
        pl.semaphore_wait(barrier, len(meets))
        bag(3 * step).start()
        bag(1).start()
        send(first)
        signal(pair_sem, (3 * step, 0))
        signal(pair_sem, (3 * step, 1))
        pl.semaphore_wait(pair_sem, 2)
        bag(3 * step + 1).start()
        send(second)

    tiles = block_len // LANES
    packed_rows = SUBLANES // per_vreg
    slot = (
        lax.rem(lax.broadcasted_iota(jnp.int32, (SUBLANES, LANES), 0), packed_rows) * per_vreg
        + lax.div(lax.broadcasted_iota(jnp.int32, (SUBLANES, LANES), 1), bag_len)
    )
    left_rows = lax.broadcasted_iota(jnp.int32, (tiles * SUBLANES, LANES), 0)
    right_rows = lax.broadcasted_iota(jnp.int32, (LANES, LANES), 0)

    def one_hot(numbers, first, against):
        return jnp.concatenate(
            [
                jnp.where(numbers[k:k + 1, :] == against, 1.0, 0.0).astype(jnp.bfloat16)
                for k in range(first, first + packed_rows)
            ],
            axis=1,
        )

    def enter():
        for mask in inner_order + near + beside + [(0, 0)]:
            load(mask).wait()

        @pl.when(inner)
        def _():
            for mask in (1, 3 * step, 3 * step + 1):
                bag(mask).wait_recv()
            pl.semaphore_wait(all_sem, 1)
            pair(step, 0).start()
            pair(half, 3 * step).start()

        @pl.when(outer)
        def _():
            pl.semaphore_wait(barrier, len(others))
            signal(all_sem, (step, 0))
            for mask in range(rows - 1, 0, -1):
                bag(mask).start()

        go(0)

    def go(n):
        @pl.when(inner)
        def _():
            send(stage(inner_order, beside, near, IN, n))

        @pl.when(outer)
        def _():
            send(stage(outer_order, beside, near, OUT, n))

    def count(turn, _):
        @pl.when(turn == 1)
        def _():
            enter()

        @pl.when(outer)
        def _():
            for n, mask in enumerate((1, 3 * step, 3 * step + 1)):
                @pl.when(turn == n + 1)
                def _():
                    bag(mask).wait_recv()

            for n, mask in ((half, step), (half + step, half)):
                @pl.when(turn == n)
                def _():
                    pair(mask, mask).wait_recv()

        @pl.when(inner)
        def _():
            for n in range(half, rows):
                @pl.when(turn == n)
                def _():
                    bag(n - step).wait_recv()

        @pl.when(turn == half)
        def _():
            go(1)

        @pl.when(turn == half + step)
        def _():
            go(2)

        mask = turn + jnp.where(turn >= half, -step, jnp.where(turn >= step, half, 0))
        group = flipped(r, mask, rows)
        shifted = gathered[group] - r * block_len
        tile = lax.shift_right_arithmetic(shifted, LANES.bit_length() - 1)
        lane = shifted - tile * LANES
        code = tile * SUBLANES + slot
        for k in range(SUBLANES // packed_rows):
            found = lax.dot_general(
                one_hot(code, k * packed_rows, left_rows),
                one_hot(lane, k * packed_rows, right_rows),
                (((1,), (1,)), ((), ())),
                preferred_element_type=jnp.float32,
            )
            row = group * own_bags + k * SUBLANES
            for t in range(tiles):
                counts[pl.ds(row, SUBLANES), t * LANES:(t + 1) * LANES] = (
                    found[t * SUBLANES:(t + 1) * SUBLANES, :]
                )
        return 0

    lax.fori_loop(0, rows, count, 0)

    @pl.when(inner)
    def _():
        for mask in (1, 3 * step, 3 * step + 1):
            bag(mask).wait_send()
        pair(step, 0).wait_send()
        pair(half, 3 * step).wait_send()

    @pl.when(outer)
    def _():
        for mask in range(1, rows):
            bag(mask).wait_send()


    go(3)
    depth = math.gcd(block_len, 512)
    partial[...] = jnp.zeros_like(partial)

    def multiply(turn, _):
        at = pl.multiple_of(turn * depth, depth)
        block = table_v[pl.ds(at, depth), :]
        times = counts[:, pl.ds(at, depth)].astype(jnp.bfloat16)
        high = block.astype(jnp.bfloat16)
        rest = block - high.astype(jnp.float32)
        middle = rest.astype(jnp.bfloat16)
        low = (rest - middle.astype(jnp.float32)).astype(jnp.bfloat16)
        dot = functools.partial(jnp.dot, preferred_element_type=jnp.float32)
        both = dot(times, jnp.concatenate([high, middle], axis=1))
        step = (dot(times, low) + both[:, width:]) + both[:, :width]
        partial[...] += step.reshape(partial.shape)
        return 0

    lax.fori_loop(0, block_len // depth, multiply, 0)

    low, high = lax.rem(r, half), lax.div(r, half)
    sum_copies = []
    for mr in range(1, half):
        pr, _ = peer((mr, 0))
        copy = pltpu.make_async_remote_copy(
            src_ref=partial.at[:, lax.rem(pr, half)], dst_ref=arrived.at[mr],
            send_sem=sum_send.at[mr], recv_sem=sum_recv.at[mr],
            device_id=(c, pr), device_id_type=MESH,
        )
        copy.start()
        sum_copies.append(copy)

    go(4)
    for copy in sum_copies:
        copy.wait()
    total = partial[:, low]
    for mr in range(1, half):
        total += arrived[mr]
    halves[...] = total
    own.wait()
    other, _ = peer((half, 0))
    across = pltpu.make_async_remote_copy(
        src_ref=halves.at[1 - high], dst_ref=crossed,
        send_sem=cross_send, recv_sem=cross_recv,
        device_id=(c, other), device_id_type=MESH,
    )
    across.start()

    go(5)
    across.wait()
    go(6)
    pooled_ref[...] = halves[high] + crossed[...]
    moved = pl.ds(0, len(others) * span)
    for sem in (send_sem, recv_sem):
        pltpu.make_async_copy(table_ref.at[moved, :], table_v.at[moved, :], sem).wait()


def stage(far, beside, near, cuts, n):
    def part(chosen, ends):
        ends = (0,) + ends + (len(chosen),)
        return chosen[ends[n]:ends[n + 1]]

    one, two, three = part(far, cuts[0]), part(beside, cuts[1]), part(near, cuts[2])
    result = []
    for k in range(max(len(one), len(two))):
        result += two[k:k + 1] + one[k:k + 1]
    return result + three


IN, OUT = ((1, 2, 3, 4, 5, 6), (1, 2, 3, 4, 5, 6), (0, 0, 0, 0, 0, 0)), ((2, 3, 4, 5, 6, 7), (1, 2, 3, 4, 5, 6), (0, 0, 0, 0, 0, 0))


def per_device(column_table, bag_rows):
    rows, cols = lax.axis_size("row"), lax.axis_size("col")
    block_len, width = column_table.shape
    own_bags, bag_len = bag_rows.shape
    span = block_len // (rows * cols)
    fits = (
        width % LANES == 0 and LANES % bag_len == 0 and bag_len * SUBLANES >= LANES and own_bags * bag_len == SUBLANES * LANES
        and span % SUBLANES == 0 and block_len % LANES == 0
        and rows // 4 == 2 and rows % 4 == 0 and cols >= 4 and cols & (cols - 1) == 0
    )
    if not fits:
        return general(column_table, bag_rows)
    bags = own_bags * rows
    half = rows // 2
    dma = pltpu.SemaphoreType.DMA
    landed, sums = pl.pallas_call(
        functools.partial(kernel, rows, cols),
        out_shape=(
            jax.ShapeDtypeStruct((rows, cols, span, width), jnp.float32),
            jax.ShapeDtypeStruct((own_bags, width), jnp.float32),
        ),
        in_specs=[pl.BlockSpec(memory_space=pltpu.HBM), pl.BlockSpec(memory_space=pltpu.HBM)],
        out_specs=(pl.BlockSpec(memory_space=pltpu.VMEM), pl.BlockSpec(memory_space=pltpu.VMEM)),
        scratch_shapes=[
            pltpu.VMEM((block_len, width), jnp.float32),
            pltpu.VMEM((own_bags, bag_len), jnp.int32),
            pltpu.VMEM((rows, SUBLANES, LANES), jnp.int32),
            pltpu.VMEM((bags, block_len), jnp.float32),
            pltpu.VMEM((2, half, own_bags, width), jnp.float32),
            pltpu.VMEM((half, 2, own_bags, width), jnp.float32),
            pltpu.VMEM((2, own_bags, width), jnp.float32),
            pltpu.VMEM((own_bags, width), jnp.float32),
            dma((rows * cols,)), dma, dma,
            pltpu.SemaphoreType.REGULAR, pltpu.SemaphoreType.REGULAR,
            dma, dma,
            dma((rows,)), dma((rows,)),
            dma((half,)), dma((half,)), dma, dma,
        ],
        compiler_params=pltpu.CompilerParams(
            collective_id=0, has_side_effects=True, vmem_limit_bytes=32 * 1024 * 1024
        ),
    )(
        pltpu.with_memory_space_constraint(column_table, pltpu.HBM),
        pltpu.with_memory_space_constraint(bag_rows, pltpu.HBM),
    )
    return pl.pallas_call(
        write_out,
        out_shape=(
            jax.ShapeDtypeStruct((rows, span, width * cols), jnp.float32),
            jax.ShapeDtypeStruct((own_bags, width), jnp.float32),
        ),
        in_specs=[pl.BlockSpec(memory_space=pltpu.VMEM)] * 2,
        out_specs=(pl.BlockSpec(memory_space=pltpu.HBM), pl.BlockSpec(memory_space=pltpu.HBM)),
        scratch_shapes=[dma((cols,)), dma],
        compiler_params=pltpu.CompilerParams(vmem_limit_bytes=8 * 1024 * 1024),
    )(landed, sums)


def write_out(landed_ref, sums_ref, out_ref, pooled_ref, sems, sum_sem):
    rows, cols, _, width = landed_ref.shape
    copies = [pltpu.make_async_copy(sums_ref, pooled_ref, sum_sem)]
    for c in range(cols):
        copies.append(pltpu.make_async_copy(
            landed_ref.at[:, c], out_ref.at[:, :, c * width:(c + 1) * width], sems.at[c]
        ))
    for copy in copies:
        copy.start()
    for copy in copies:
        copy.wait()


def solution(mesh):
    return jax.shard_map(
        per_device,
        mesh=mesh,
        in_specs=(P("row", "col"), P("row", None)),
        out_specs=(P(None, ("col", "row"), None), P("row", "col")),
        check_vma=False,
    )
```

```python
import functools
import math

import jax
import jax.numpy as jnp
from jax import lax
from jax.experimental import pallas as pl
from jax.experimental.pallas import tpu as pltpu
from jax.sharding import PartitionSpec as P

MESH = pl.DeviceIdType.MESH
LANES = 128
SUBLANES = 8


def pooling(positions, table_rows):
    row_count = table_rows.shape[0]
    bag_count = positions.shape[0]
    block_rows = math.gcd(row_count, 512)
    turns = row_count // block_rows
    running = jnp.zeros((bag_count, table_rows.shape[1]), jnp.float32)
    tile_ids = jnp.arange(block_rows, dtype=jnp.int32)

    def advance(turn, carried):
        offset = turn * block_rows
        within = positions - offset
        matches = within[:, :, None] == tile_ids[None, None, :]
        counts = jnp.sum(matches.astype(jnp.float32), axis=1)
        table_block = lax.dynamic_slice_in_dim(table_rows, offset, block_rows, 0)
        return carried + jnp.dot(
            counts, table_block, precision=lax.Precision.HIGHEST, preferred_element_type=jnp.float32
        )

    return lax.fori_loop(0, turns, advance, running)


def general(column_table, bag_rows):
    row_groups = lax.axis_size("row")
    col_groups = lax.axis_size("col")
    block_len, col_width = column_table.shape
    full_width = col_width * col_groups
    span = block_len // (col_groups * row_groups)
    row_index = lax.axis_index("row")
    every_bag = lax.all_gather(bag_rows, "row", axis=0, tiled=True)
    sectioned = column_table.reshape(col_groups, row_groups, span, col_width)
    moved = lax.all_to_all(
        lax.all_to_all(sectioned, "col", split_axis=0, concat_axis=3, tiled=True),
        "row",
        split_axis=1,
        concat_axis=0,
        tiled=True,
    )
    row_table = moved.reshape(row_groups, span, full_width)
    first_row = row_index * block_len
    shifted = every_bag - first_row
    inside = (shifted >= 0) & (shifted < block_len)
    positions = jnp.where(inside, shifted, -1)
    pooled = lax.psum_scatter(
        pooling(positions, column_table), "row", scatter_dimension=0, tiled=True
    )
    return (row_table, pooled)


def flipped(index, mask, count):
    result, bit = 0, 1
    while bit < count:
        total = lax.div(index, bit) + (mask // bit if isinstance(mask, int) else lax.div(mask, bit))
        result = result + lax.rem(total, 2) * bit
        bit *= 2
    return result


def orders(rows, cols):
    step, half, across = rows // 4, rows // 2, cols // 2
    masks = [(mr, mc) for mr in range(rows) for mc in range(cols)]
    spread = lambda m: -((m[0] % step > 0) + (m[1] >= across))
    first = [(3 * step, 0)]
    second = [(3 * step + 1, 0), (3 * step + 1, 1), (3 * step, across), (3 * step, across + 1)]
    last = (3 * step, 1)
    near = [m for m in masks if m[0] < step and m != (0, 0)]
    beside = [m for m in masks if step <= m[0] < half]
    two = sorted((m for m in masks if half <= m[0] < 3 * step), key=spread)
    three = sorted((m for m in masks if m[0] >= 3 * step), key=spread)
    left = [m for m in three if m not in first + second + [last]]
    inner = two + left + [last]
    outer = two + three
    return first, second, inner, outer, near, beside


def kernel(
    row_groups, col_groups,
    table_ref, bags_ref, out_ref, pooled_ref,
    table_v, bags_v, gathered, counts, partial, arrived, halves, crossed,
    load_sem, bag_sem, own_sem, pair_sem, all_sem, send_sem, recv_sem,
    bag_send, bag_recv, sum_send, sum_recv, cross_send, cross_recv,
):
    rows, cols = row_groups, col_groups
    r, c = lax.axis_index("row"), lax.axis_index("col")
    block_len, width = table_ref.shape
    span = block_len // (rows * cols)
    own_bags, bag_len = bags_ref.shape
    per_vreg = LANES // bag_len
    half, step = rows // 2, rows // 4
    plane = lax.div(r, step)
    inner = (plane == 1) | (plane == 2)
    outer = (plane == 0) | (plane == 3)

    first, second, inner_order, outer_order, near, beside = orders(rows, cols)
    masks = [(mr, mc) for mr in range(rows) for mc in range(cols)]
    others = [m for m in masks if m != (0, 0)]
    meets = first + [(3 * step, 1), (1, 0), (0, cols // 2)]

    def peer(mask):
        return flipped(r, mask[0], rows), flipped(c, mask[1], cols)

    def at(mask):
        pr, pc = peer(mask)
        return pl.ds((pc * rows + pr) * span, span)

    def signal(sem, mask):
        pr, pc = peer(mask)
        pl.semaphore_signal(sem, inc=1, device_id=(pc, pr), device_id_type=MESH)

    def load(chosen, sem):
        for mask in chosen:
            pltpu.make_async_copy(table_ref.at[at(mask), :], table_v.at[at(mask), :], sem).start()

    def chunks(count, sem):
        whole = pl.ds(0, count * span)
        pltpu.make_async_copy(table_ref.at[whole, :], table_v.at[whole, :], sem).wait()

    def bulk(mask):
        pr, pc = peer(mask)
        return pltpu.make_async_remote_copy(
            src_ref=table_v.at[at(mask), :], dst_ref=out_ref.at[r, c],
            send_sem=send_sem, recv_sem=recv_sem,
            device_id=(pc, pr), device_id_type=MESH,
        )

    def send(chosen):
        for mask in chosen:
            bulk(mask).start()

    bag_load = pltpu.make_async_copy(bags_ref, bags_v, bag_sem)
    bag_load.start()
    barrier = pltpu.get_barrier_semaphore()

    @pl.when(inner)
    def _():
        for mask in meets:
            signal(barrier, mask)

    load(first, load_sem.at[0])
    load(second, load_sem.at[1])

    @pl.when(inner)
    def _():
        for mask in others:
            if mask[0] // step in (1, 2):
                signal(barrier, mask)

    @pl.when(outer)
    def _():
        for mask in others:
            if mask[0] // step in (0, 3):
                signal(barrier, mask)

    rest = inner_order + near + beside + [(0, 0)]
    load(rest, load_sem.at[2])
    own = pltpu.make_async_copy(table_ref.at[at((0, 0)), :], out_ref.at[r, c], own_sem)
    own.start()

    def bag(mask, kind):
        pr, _ = peer((mask, 0))
        return pltpu.make_async_remote_copy(
            src_ref=gathered.at[r], dst_ref=gathered.at[r],
            send_sem=bag_send, recv_sem=bag_recv.at[kind],
            device_id=(c, pr), device_id_type=MESH,
        )

    def pair(source):
        kind = 1
        pr, _ = peer((step, 0))
        rows_of = pl.ds(lax.div(flipped(r, source, rows), step) * step, step)
        return pltpu.make_async_remote_copy(
            src_ref=gathered.at[rows_of], dst_ref=gathered.at[rows_of],
            send_sem=bag_send, recv_sem=bag_recv.at[kind],
            device_id=(c, pr), device_id_type=MESH,
        )

    def bags(count, sem):
        whole = gathered.at[pl.ds(0, count)]
        pltpu.make_async_remote_copy(
            src_ref=whole, dst_ref=whole, send_sem=bag_send, recv_sem=sem,
            device_id=peer((1, 0))[::-1], device_id_type=MESH,
        ).wait_recv()

    bag_load.wait()
    gathered[r] = jnp.concatenate(
        [bags_v[pl.ds(q, SUBLANES, stride=per_vreg), :] for q in range(per_vreg)], axis=1
    )
    chunks(len(first), load_sem.at[0])

    @pl.when(inner)
    def _():
        pl.semaphore_wait(barrier, len(meets))
        bag(3 * step, 0).start()
        bag(1, 0).start()
        send(first)
        signal(pair_sem, (3 * step, 0))
        signal(pair_sem, (3 * step, 1))
        chunks(len(second), load_sem.at[1])
        pl.semaphore_wait(pair_sem, 2)
        bag(3 * step + 1, 0).start()
        send(second)

    tiles = block_len // LANES
    packed_rows = SUBLANES // per_vreg
    slot = (
        lax.rem(lax.broadcasted_iota(jnp.int32, (SUBLANES, LANES), 0), packed_rows) * per_vreg
        + lax.div(lax.broadcasted_iota(jnp.int32, (SUBLANES, LANES), 1), bag_len)
    )
    left_rows = lax.broadcasted_iota(jnp.int32, (tiles * SUBLANES, LANES), 0)
    right_rows = lax.broadcasted_iota(jnp.int32, (LANES, LANES), 0)

    def one_hot(numbers, first, against):
        return jnp.concatenate(
            [
                jnp.where(numbers[k:k + 1, :] == against, 1.0, 0.0).astype(jnp.bfloat16)
                for k in range(first, first + packed_rows)
            ],
            axis=1,
        )

    def enter():
        chunks(len(rest), load_sem.at[2])

        @pl.when(inner)
        def _():
            bags(half - 1, bag_recv.at[0])
            pl.semaphore_wait(all_sem, 1)
            pair(0).start()
            pair(3 * step).start()

        @pl.when(outer)
        def _():
            chunks(len(second), load_sem.at[1])
            pl.semaphore_wait(barrier, len(others))
            signal(all_sem, (step, 0))
            for mask in range(rows - 1, 0, -1):
                bag(mask, 0 if mask < step or mask >= 3 * step else 1).start()

        go(0)

    def go(n):
        @pl.when(inner)
        def _():
            send(stage(inner_order, beside, near, IN, n))

        @pl.when(outer)
        def _():
            send(stage(outer_order, beside, near, OUT, n))

    def count(turn, _):
        @pl.when(turn == 1)
        def _():
            enter()

        @pl.when((turn == 1) & outer)
        def _():
            bags(half - 1, bag_recv.at[0])

        @pl.when(turn == half)
        def _():
            bags(half, bag_recv.at[1])
            go(1)

        @pl.when(turn == half + step)
        def _():
            go(2)

        mask = turn + jnp.where(turn >= half, -step, jnp.where(turn >= step, half, 0))
        group = flipped(r, mask, rows)
        shifted = gathered[group] - r * block_len
        tile = lax.shift_right_arithmetic(shifted, LANES.bit_length() - 1)
        lane = shifted - tile * LANES
        code = tile * SUBLANES + slot
        for k in range(SUBLANES // packed_rows):
            found = lax.dot_general(
                one_hot(code, k * packed_rows, left_rows),
                one_hot(lane, k * packed_rows, right_rows),
                (((1,), (1,)), ((), ())),
                preferred_element_type=jnp.float32,
            )
            row = group * own_bags + k * SUBLANES
            for t in range(tiles):
                counts[pl.ds(row, SUBLANES), t * LANES:(t + 1) * LANES] = (
                    found[t * SUBLANES:(t + 1) * SUBLANES, :]
                )
        return 0

    lax.fori_loop(0, rows, count, 0)

    bags(rows - 1, bag_send)

    go(3)
    depth = math.gcd(block_len, 512)
    partial[...] = jnp.zeros_like(partial)

    def multiply(turn, _):
        at = pl.multiple_of(turn * depth, depth)
        block = table_v[pl.ds(at, depth), :]
        times = counts[:, pl.ds(at, depth)].astype(jnp.bfloat16)
        high = block.astype(jnp.bfloat16)
        rest = block - high.astype(jnp.float32)
        middle = rest.astype(jnp.bfloat16)
        low = (rest - middle.astype(jnp.float32)).astype(jnp.bfloat16)
        dot = functools.partial(jnp.dot, preferred_element_type=jnp.float32)
        both = dot(times, jnp.concatenate([high, middle], axis=1))
        step = (dot(times, low) + both[:, width:]) + both[:, :width]
        partial[...] += step.reshape(partial.shape)
        return 0

    lax.fori_loop(0, block_len // depth, multiply, 0)

    low, high = lax.rem(r, half), lax.div(r, half)
    for mr in range(1, half):
        pr, _ = peer((mr, 0))
        copy = pltpu.make_async_remote_copy(
            src_ref=partial.at[:, lax.rem(pr, half)], dst_ref=arrived.at[mr],
            send_sem=sum_send, recv_sem=sum_recv,
            device_id=(c, pr), device_id_type=MESH,
        )
        copy.start()

    go(4)
    for sem in (sum_send, sum_recv):
        pltpu.make_async_copy(arrived.at[pl.ds(1, half - 1)], arrived.at[pl.ds(1, half - 1)], sem).wait()
    total = partial[:, low]
    for mr in range(1, half):
        total += arrived[mr]
    halves[...] = total
    own.wait()
    other, _ = peer((half, 0))
    across = pltpu.make_async_remote_copy(
        src_ref=halves.at[1 - high], dst_ref=crossed,
        send_sem=cross_send, recv_sem=cross_recv,
        device_id=(c, other), device_id_type=MESH,
    )
    across.start()

    go(5)
    across.wait()
    go(6)
    pooled_ref[...] = halves[high] + crossed[...]
    moved = pl.ds(0, len(others) * span)
    for sem in (send_sem, recv_sem):
        pltpu.make_async_copy(table_ref.at[moved, :], table_v.at[moved, :], sem).wait()


def stage(far, beside, near, cuts, n):
    def part(chosen, ends):
        ends = (0,) + ends + (len(chosen),)
        return chosen[ends[n]:ends[n + 1]]

    one, two, three = part(far, cuts[0]), part(beside, cuts[1]), part(near, cuts[2])
    result = []
    for k in range(max(len(one), len(two))):
        result += two[k:k + 1] + one[k:k + 1]
    return result + three


IN = (5, 5, 5, 5, 5, 11), (0, 0, 0, 0, 8, 8), (0, 0, 0, 0, 0, 7)
OUT = (0, 0, 0, 0, 4, 16), (2, 2, 2, 2, 4, 8), (3, 3, 3, 3, 7, 7)


def per_device(column_table, bag_rows):
    rows, cols = lax.axis_size("row"), lax.axis_size("col")
    block_len, width = column_table.shape
    own_bags, bag_len = bag_rows.shape
    span = block_len // (rows * cols)
    fits = (
        width % LANES == 0 and LANES % bag_len == 0 and bag_len * SUBLANES >= LANES and own_bags * bag_len == SUBLANES * LANES
        and span % SUBLANES == 0 and block_len % LANES == 0
        and rows // 4 == 2 and rows % 4 == 0 and cols >= 4 and cols & (cols - 1) == 0
    )
    if not fits:
        return general(column_table, bag_rows)
    bags = own_bags * rows
    half = rows // 2
    dma = pltpu.SemaphoreType.DMA
    landed, sums = pl.pallas_call(
        functools.partial(kernel, rows, cols),
        out_shape=(
            jax.ShapeDtypeStruct((rows, cols, span, width), jnp.float32),
            jax.ShapeDtypeStruct((own_bags, width), jnp.float32),
        ),
        in_specs=[pl.BlockSpec(memory_space=pltpu.HBM), pl.BlockSpec(memory_space=pltpu.HBM)],
        out_specs=(pl.BlockSpec(memory_space=pltpu.VMEM), pl.BlockSpec(memory_space=pltpu.VMEM)),
        scratch_shapes=[
            pltpu.VMEM((block_len, width), jnp.float32),
            pltpu.VMEM((own_bags, bag_len), jnp.int32),
            pltpu.VMEM((rows, SUBLANES, LANES), jnp.int32),
            pltpu.VMEM((bags, block_len), jnp.float32),
            pltpu.VMEM((2, half, own_bags, width), jnp.float32),
            pltpu.VMEM((half, 2, own_bags, width), jnp.float32),
            pltpu.VMEM((2, own_bags, width), jnp.float32),
            pltpu.VMEM((own_bags, width), jnp.float32),
            dma((3,)), dma, dma,
            pltpu.SemaphoreType.REGULAR, pltpu.SemaphoreType.REGULAR,
            dma, dma,
            dma, dma((2,)), dma, dma, dma, dma,
        ],
        compiler_params=pltpu.CompilerParams(
            collective_id=0, has_side_effects=True, vmem_limit_bytes=32 * 1024 * 1024
        ),
    )(
        pltpu.with_memory_space_constraint(column_table, pltpu.HBM),
        pltpu.with_memory_space_constraint(bag_rows, pltpu.HBM),
    )
    return pl.pallas_call(
        write_out,
        out_shape=(
            jax.ShapeDtypeStruct((rows, span, width * cols), jnp.float32),
            jax.ShapeDtypeStruct((own_bags, width), jnp.float32),
        ),
        in_specs=[pl.BlockSpec(memory_space=pltpu.VMEM)] * 2,
        out_specs=(pl.BlockSpec(memory_space=pltpu.HBM), pl.BlockSpec(memory_space=pltpu.HBM)),
        scratch_shapes=[dma((cols,)), dma],
        compiler_params=pltpu.CompilerParams(vmem_limit_bytes=8 * 1024 * 1024),
    )(landed, sums)


def write_out(landed_ref, sums_ref, out_ref, pooled_ref, sems, sum_sem):
    rows, cols, _, width = landed_ref.shape
    copies = [pltpu.make_async_copy(sums_ref, pooled_ref, sum_sem)]
    for c in range(cols):
        copies.append(pltpu.make_async_copy(
            landed_ref.at[:, c], out_ref.at[:, :, c * width:(c + 1) * width], sems.at[c]
        ))
    for copy in copies:
        copy.start()
    for copy in copies:
        copy.wait()


def solution(mesh):
    return jax.shard_map(
        per_device,
        mesh=mesh,
        in_specs=(P("row", "col"), P("row", None)),
        out_specs=(P(None, ("col", "row"), None), P("row", "col")),
        check_vma=False,
    )
```

```python
import functools
import math

import jax
import jax.numpy as jnp
from jax import lax
from jax.experimental import pallas as pl
from jax.experimental.pallas import tpu as pltpu
from jax.sharding import PartitionSpec as P

MESH = pl.DeviceIdType.MESH
LANES = 128
SUBLANES = 8


def pooling(positions, table_rows):
    row_count = table_rows.shape[0]
    bag_count = positions.shape[0]
    block_rows = math.gcd(row_count, 512)
    turns = row_count // block_rows
    running = jnp.zeros((bag_count, table_rows.shape[1]), jnp.float32)
    tile_ids = jnp.arange(block_rows, dtype=jnp.int32)

    def advance(turn, carried):
        offset = turn * block_rows
        within = positions - offset
        matches = within[:, :, None] == tile_ids[None, None, :]
        counts = jnp.sum(matches.astype(jnp.float32), axis=1)
        table_block = lax.dynamic_slice_in_dim(table_rows, offset, block_rows, 0)
        return carried + jnp.dot(
            counts, table_block, precision=lax.Precision.HIGHEST, preferred_element_type=jnp.float32
        )

    return lax.fori_loop(0, turns, advance, running)


def general(column_table, bag_rows):
    row_groups = lax.axis_size("row")
    col_groups = lax.axis_size("col")
    block_len, col_width = column_table.shape
    full_width = col_width * col_groups
    span = block_len // (col_groups * row_groups)
    row_index = lax.axis_index("row")
    every_bag = lax.all_gather(bag_rows, "row", axis=0, tiled=True)
    sectioned = column_table.reshape(col_groups, row_groups, span, col_width)
    moved = lax.all_to_all(
        lax.all_to_all(sectioned, "col", split_axis=0, concat_axis=3, tiled=True),
        "row",
        split_axis=1,
        concat_axis=0,
        tiled=True,
    )
    row_table = moved.reshape(row_groups, span, full_width)
    first_row = row_index * block_len
    shifted = every_bag - first_row
    inside = (shifted >= 0) & (shifted < block_len)
    positions = jnp.where(inside, shifted, -1)
    pooled = lax.psum_scatter(
        pooling(positions, column_table), "row", scatter_dimension=0, tiled=True
    )
    return (row_table, pooled)


def flipped(index, mask, count):
    result, bit = 0, 1
    while bit < count:
        total = lax.div(index, bit) + (mask // bit if isinstance(mask, int) else lax.div(mask, bit))
        result = result + lax.rem(total, 2) * bit
        bit *= 2
    return result


def orders(rows, cols):
    step, half, across = rows // 4, rows // 2, cols // 2
    masks = [(mr, mc) for mr in range(rows) for mc in range(cols)]
    spread = lambda m: -((m[0] % step > 0) + (m[1] >= across))
    first = [(3 * step, 0)]
    second = [(3 * step + 1, 0), (3 * step + 1, 1), (3 * step, across), (3 * step, across + 1)]
    last = (3 * step, 1)
    near = [m for m in masks if m[0] < step and m != (0, 0)]
    beside = [m for m in masks if step <= m[0] < half]
    two = sorted((m for m in masks if half <= m[0] < 3 * step), key=spread)
    three = sorted((m for m in masks if m[0] >= 3 * step), key=spread)
    left = [m for m in three if m not in first + second + [last]]
    mixed = [m for pair in zip(two, three) for m in pair]
    far = [mixed, two + left + [last], two + left + [last], two + three]
    return first, second, far, near, beside


def kernel(
    row_groups, col_groups,
    table_ref, bags_ref, out_ref, pooled_ref,
    table_v, bags_v, gathered, counts, partial, arrived, halves, crossed,
    load_sem, bag_sem, own_sem, pair_sem, all_sem, send_sem, recv_sem,
    bag_send, bag_recv, sum_send, sum_recv, cross_send, cross_recv,
):
    rows, cols = row_groups, col_groups
    r, c = lax.axis_index("row"), lax.axis_index("col")
    block_len, width = table_ref.shape
    span = block_len // (rows * cols)
    own_bags, bag_len = bags_ref.shape
    per_vreg = LANES // bag_len
    half, step = rows // 2, rows // 4
    plane = lax.div(r, step)
    inner = (plane == 1) | (plane == 2)
    outer = (plane == 0) | (plane == 3)

    first, second, far, near, beside = orders(rows, cols)
    masks = [(mr, mc) for mr in range(rows) for mc in range(cols)]
    others = [m for m in masks if m != (0, 0)]
    meets = [(3 * step, 0), (3 * step, 1), (1, 0), (0, cols // 2)]

    def peer(mask):
        return flipped(r, mask[0], rows), flipped(c, mask[1], cols)

    def at(mask):
        pr, pc = peer(mask)
        return pl.ds((pc * rows + pr) * span, span)

    def signal(sem, mask):
        pr, pc = peer(mask)
        pl.semaphore_signal(sem, inc=1, device_id=(pc, pr), device_id_type=MESH)

    def load(chosen, sem):
        for mask in chosen:
            pltpu.make_async_copy(table_ref.at[at(mask), :], table_v.at[at(mask), :], sem).start()

    def chunks(count, sem):
        whole = pl.ds(0, count * span)
        pltpu.make_async_copy(table_ref.at[whole, :], table_v.at[whole, :], sem).wait()

    def bulk(mask):
        pr, pc = peer(mask)
        return pltpu.make_async_remote_copy(
            src_ref=table_v.at[at(mask), :], dst_ref=out_ref.at[r, c],
            send_sem=send_sem, recv_sem=recv_sem,
            device_id=(pc, pr), device_id_type=MESH,
        )

    def send(chosen):
        for mask in chosen:
            bulk(mask).start()

    bag_load = pltpu.make_async_copy(bags_ref, bags_v, bag_sem)
    bag_load.start()
    barrier = pltpu.get_barrier_semaphore()

    @pl.when(inner)
    def _():
        for mask in meets:
            signal(barrier, mask)

    load(first, load_sem.at[0])
    load(second, load_sem.at[1])

    @pl.when(inner)
    def _():
        for mask in others:
            if mask[0] // step in (1, 2):
                signal(barrier, mask)

    @pl.when(outer)
    def _():
        for mask in others:
            if mask[0] // step in (0, 3):
                signal(barrier, mask)

    rest = far[1] + near + beside + [(0, 0)]
    load(rest, load_sem.at[2])
    own = pltpu.make_async_copy(table_ref.at[at((0, 0)), :], out_ref.at[r, c], own_sem)
    own.start()

    def bag(mask, kind):
        pr, _ = peer((mask, 0))
        return pltpu.make_async_remote_copy(
            src_ref=gathered.at[r], dst_ref=gathered.at[r],
            send_sem=bag_send, recv_sem=bag_recv.at[kind],
            device_id=(c, pr), device_id_type=MESH,
        )

    def pair(source):
        kind = 1
        pr, _ = peer((step, 0))
        rows_of = pl.ds(lax.div(flipped(r, source, rows), step) * step, step)
        return pltpu.make_async_remote_copy(
            src_ref=gathered.at[rows_of], dst_ref=gathered.at[rows_of],
            send_sem=bag_send, recv_sem=bag_recv.at[kind],
            device_id=(c, pr), device_id_type=MESH,
        )

    def bags(count, sem):
        whole = gathered.at[pl.ds(0, count)]
        pltpu.make_async_remote_copy(
            src_ref=whole, dst_ref=whole, send_sem=bag_send, recv_sem=sem,
            device_id=peer((1, 0))[::-1], device_id_type=MESH,
        ).wait_recv()

    bag_load.wait()
    gathered[r] = jnp.concatenate(
        [bags_v[pl.ds(q, SUBLANES, stride=per_vreg), :] for q in range(per_vreg)], axis=1
    )
    chunks(len(first), load_sem.at[0])

    @pl.when(inner)
    def _():
        pl.semaphore_wait(barrier, len(meets))
        bag(3 * step, 0).start()
        bag(1, 0).start()
        send(first)
        signal(pair_sem, (3 * step, 0))
        signal(pair_sem, (3 * step, 1))
        chunks(len(second), load_sem.at[1])
        pl.semaphore_wait(pair_sem, 2)
        bag(3 * step + 1, 0).start()
        send(second)

    tiles = block_len // LANES
    packed_rows = SUBLANES // per_vreg
    slot = (
        lax.rem(lax.broadcasted_iota(jnp.int32, (SUBLANES, LANES), 0), packed_rows) * per_vreg
        + lax.div(lax.broadcasted_iota(jnp.int32, (SUBLANES, LANES), 1), bag_len)
    )
    left_rows = lax.broadcasted_iota(jnp.int32, (tiles * SUBLANES, LANES), 0)
    right_rows = lax.broadcasted_iota(jnp.int32, (LANES, LANES), 0)

    def one_hot(numbers, first, against):
        return jnp.concatenate(
            [
                jnp.where(numbers[k:k + 1, :] == against, 1.0, 0.0).astype(jnp.bfloat16)
                for k in range(first, first + packed_rows)
            ],
            axis=1,
        )

    def enter():
        chunks(len(rest), load_sem.at[2])

        @pl.when(inner)
        def _():
            bags(half - 1, bag_recv.at[0])
            pl.semaphore_wait(all_sem, 1)
            pair(0).start()
            pair(3 * step).start()

        @pl.when(outer)
        def _():
            chunks(len(second), load_sem.at[1])
            pl.semaphore_wait(barrier, len(others))
            signal(all_sem, (step, 0))
            for mask in range(rows - 1, 0, -1):
                bag(mask, 0 if mask < step or mask >= 3 * step else 1).start()

        go(0)

    def go(n):
        for place in range(4):
            @pl.when(plane == place)
            def _():
                send(stage(far[place], beside, near, CUTS[place], n))

    def count(turn, _):
        @pl.when(turn == 1)
        def _():
            enter()

        @pl.when((turn == 1) & outer)
        def _():
            bags(half - 1, bag_recv.at[0])

        @pl.when(turn == half)
        def _():
            bags(half, bag_recv.at[1])
            go(1)

        @pl.when(turn == half + step)
        def _():
            go(2)

        mask = turn + jnp.where(turn >= half, -step, jnp.where(turn >= step, half, 0))
        group = flipped(r, mask, rows)
        shifted = gathered[group] - r * block_len
        tile = lax.shift_right_arithmetic(shifted, LANES.bit_length() - 1)
        lane = shifted - tile * LANES
        code = tile * SUBLANES + slot
        for k in range(SUBLANES // packed_rows):
            found = lax.dot_general(
                one_hot(code, k * packed_rows, left_rows),
                one_hot(lane, k * packed_rows, right_rows),
                (((1,), (1,)), ((), ())),
                preferred_element_type=jnp.float32,
            )
            row = group * own_bags + k * SUBLANES
            for t in range(tiles):
                counts[pl.ds(row, SUBLANES), t * LANES:(t + 1) * LANES] = (
                    found[t * SUBLANES:(t + 1) * SUBLANES, :]
                )
        return 0

    lax.fori_loop(0, rows, count, 0)

    bags(rows - 1, bag_send)

    go(3)
    depth = math.gcd(block_len, 512)
    partial[...] = jnp.zeros_like(partial)

    def multiply(turn, _):
        at = pl.multiple_of(turn * depth, depth)
        block = table_v[pl.ds(at, depth), :]
        times = counts[:, pl.ds(at, depth)].astype(jnp.bfloat16)
        high = block.astype(jnp.bfloat16)
        rest = block - high.astype(jnp.float32)
        middle = rest.astype(jnp.bfloat16)
        low = (rest - middle.astype(jnp.float32)).astype(jnp.bfloat16)
        dot = functools.partial(jnp.dot, preferred_element_type=jnp.float32)
        both = dot(times, jnp.concatenate([high, middle], axis=1))
        step = (dot(times, low) + both[:, width:]) + both[:, :width]
        partial[...] += step.reshape(partial.shape)
        return 0

    lax.fori_loop(0, block_len // depth, multiply, 0)

    low, high = lax.rem(r, half), lax.div(r, half)
    for mr in range(1, half):
        pr, _ = peer((mr, 0))
        copy = pltpu.make_async_remote_copy(
            src_ref=partial.at[:, lax.rem(pr, half)], dst_ref=arrived.at[mr],
            send_sem=sum_send, recv_sem=sum_recv,
            device_id=(c, pr), device_id_type=MESH,
        )
        copy.start()

    go(4)
    sent = arrived.at[pl.ds(1, half - 1)]
    pltpu.make_async_copy(sent, sent, sum_recv).wait()
    total = partial[:, low]
    for mr in range(1, half):
        total += arrived[mr]
    halves[...] = total
    own.wait()
    other, _ = peer((half, 0))
    across = pltpu.make_async_remote_copy(
        src_ref=halves.at[1 - high], dst_ref=crossed,
        send_sem=cross_send, recv_sem=cross_recv,
        device_id=(c, other), device_id_type=MESH,
    )
    across.start()

    go(5)
    across.wait()
    go(6)
    pooled_ref[...] = halves[high] + crossed[...]
    pltpu.make_async_copy(sent, sent, sum_send).wait()
    moved = pl.ds(0, len(others) * span)
    for sem in (send_sem, recv_sem):
        pltpu.make_async_copy(table_ref.at[moved, :], table_v.at[moved, :], sem).wait()


def stage(far, beside, near, cuts, n):
    def part(chosen, ends):
        ends = (0,) + ends + (len(chosen),)
        return chosen[ends[n]:ends[n + 1]]

    one, two, three = part(far, cuts[0]), part(beside, cuts[1]), part(near, cuts[2])
    spread = [((k + 0.5) / len(chosen), m) for chosen in (two, one) for k, m in enumerate(chosen)]
    result = [m for _, m in sorted(spread, key=lambda p: p[0])]
    return result + three


INNER = (5, 5, 5, 5, 5, 11), (1, 1, 1, 1, 8, 8), (0, 0, 0, 0, 0, 7)
OUTER = (0, 0, 0, 0, 4, 16), (2, 2, 2, 2, 4, 8), (3, 3, 3, 3, 7, 7)
CUTS = OUTER, INNER, INNER, OUTER


def per_device(column_table, bag_rows):
    rows, cols = lax.axis_size("row"), lax.axis_size("col")
    block_len, width = column_table.shape
    own_bags, bag_len = bag_rows.shape
    span = block_len // (rows * cols)
    fits = (
        width % LANES == 0 and LANES % bag_len == 0 and bag_len * SUBLANES >= LANES and own_bags * bag_len == SUBLANES * LANES
        and span % SUBLANES == 0 and block_len % LANES == 0
        and rows // 4 == 2 and rows % 4 == 0 and cols >= 4 and cols & (cols - 1) == 0
    )
    if not fits:
        return general(column_table, bag_rows)
    bags = own_bags * rows
    half = rows // 2
    dma = pltpu.SemaphoreType.DMA
    landed, sums = pl.pallas_call(
        functools.partial(kernel, rows, cols),
        out_shape=(
            jax.ShapeDtypeStruct((rows, cols, span, width), jnp.float32),
            jax.ShapeDtypeStruct((own_bags, width), jnp.float32),
        ),
        in_specs=[pl.BlockSpec(memory_space=pltpu.HBM), pl.BlockSpec(memory_space=pltpu.HBM)],
        out_specs=(pl.BlockSpec(memory_space=pltpu.VMEM), pl.BlockSpec(memory_space=pltpu.VMEM)),
        scratch_shapes=[
            pltpu.VMEM((block_len, width), jnp.float32),
            pltpu.VMEM((own_bags, bag_len), jnp.int32),
            pltpu.VMEM((rows, SUBLANES, LANES), jnp.int32),
            pltpu.VMEM((bags, block_len), jnp.float32),
            pltpu.VMEM((2, half, own_bags, width), jnp.float32),
            pltpu.VMEM((half, 2, own_bags, width), jnp.float32),
            pltpu.VMEM((2, own_bags, width), jnp.float32),
            pltpu.VMEM((own_bags, width), jnp.float32),
            dma((3,)), dma, dma,
            pltpu.SemaphoreType.REGULAR, pltpu.SemaphoreType.REGULAR,
            dma, dma,
            dma, dma((2,)), dma, dma, dma, dma,
        ],
        compiler_params=pltpu.CompilerParams(
            collective_id=0, has_side_effects=True, vmem_limit_bytes=32 * 1024 * 1024
        ),
    )(
        pltpu.with_memory_space_constraint(column_table, pltpu.HBM),
        pltpu.with_memory_space_constraint(bag_rows, pltpu.HBM),
    )
    return pl.pallas_call(
        write_out,
        out_shape=(
            jax.ShapeDtypeStruct((rows, span, width * cols), jnp.float32),
            jax.ShapeDtypeStruct((own_bags, width), jnp.float32),
        ),
        in_specs=[pl.BlockSpec(memory_space=pltpu.VMEM)] * 2,
        out_specs=(pl.BlockSpec(memory_space=pltpu.HBM), pl.BlockSpec(memory_space=pltpu.HBM)),
        scratch_shapes=[dma((cols,)), dma],
        compiler_params=pltpu.CompilerParams(vmem_limit_bytes=8 * 1024 * 1024),
    )(landed, sums)


def write_out(landed_ref, sums_ref, out_ref, pooled_ref, sems, sum_sem):
    rows, cols, _, width = landed_ref.shape
    copies = [pltpu.make_async_copy(sums_ref, pooled_ref, sum_sem)]
    for c in range(cols):
        copies.append(pltpu.make_async_copy(
            landed_ref.at[:, c], out_ref.at[:, :, c * width:(c + 1) * width], sems.at[c]
        ))
    for copy in copies:
        copy.start()
    for copy in copies:
        copy.wait()


def solution(mesh):
    return jax.shard_map(
        per_device,
        mesh=mesh,
        in_specs=(P("row", "col"), P("row", None)),
        out_specs=(P(None, ("col", "row"), None), P("row", "col")),
        check_vma=False,
    )
```

```python
import functools
import math

import jax
import jax.numpy as jnp
from jax import lax
from jax.experimental import pallas as pl
from jax.experimental.pallas import tpu as pltpu
from jax.sharding import PartitionSpec as P

MESH = pl.DeviceIdType.MESH
LANES = 128
SUBLANES = 8


def pooling(positions, table_rows):
    row_count = table_rows.shape[0]
    bag_count = positions.shape[0]
    block_rows = math.gcd(row_count, 512)
    turns = row_count // block_rows
    running = jnp.zeros((bag_count, table_rows.shape[1]), jnp.float32)
    tile_ids = jnp.arange(block_rows, dtype=jnp.int32)

    def advance(turn, carried):
        offset = turn * block_rows
        within = positions - offset
        matches = within[:, :, None] == tile_ids[None, None, :]
        counts = jnp.sum(matches.astype(jnp.float32), axis=1)
        table_block = lax.dynamic_slice_in_dim(table_rows, offset, block_rows, 0)
        return carried + jnp.dot(
            counts, table_block, precision=lax.Precision.HIGHEST, preferred_element_type=jnp.float32
        )

    return lax.fori_loop(0, turns, advance, running)


def general(column_table, bag_rows):
    row_groups = lax.axis_size("row")
    col_groups = lax.axis_size("col")
    block_len, col_width = column_table.shape
    full_width = col_width * col_groups
    span = block_len // (col_groups * row_groups)
    row_index = lax.axis_index("row")
    every_bag = lax.all_gather(bag_rows, "row", axis=0, tiled=True)
    sectioned = column_table.reshape(col_groups, row_groups, span, col_width)
    moved = lax.all_to_all(
        lax.all_to_all(sectioned, "col", split_axis=0, concat_axis=3, tiled=True),
        "row",
        split_axis=1,
        concat_axis=0,
        tiled=True,
    )
    row_table = moved.reshape(row_groups, span, full_width)
    first_row = row_index * block_len
    shifted = every_bag - first_row
    inside = (shifted >= 0) & (shifted < block_len)
    positions = jnp.where(inside, shifted, -1)
    pooled = lax.psum_scatter(
        pooling(positions, column_table), "row", scatter_dimension=0, tiled=True
    )
    return (row_table, pooled)


def flipped(index, mask, count):
    result, bit = 0, 1
    while bit < count:
        total = lax.div(index, bit) + (mask // bit if isinstance(mask, int) else lax.div(mask, bit))
        result = result + lax.rem(total, 2) * bit
        bit *= 2
    return result


def orders(rows, cols):
    step, half, across = rows // 4, rows // 2, cols // 2
    masks = [(mr, mc) for mr in range(rows) for mc in range(cols)]
    spread = lambda m: -((m[0] % step > 0) + (m[1] >= across))
    first = [(3 * step, 0)]
    second = [(3 * step + 1, 0), (3 * step + 1, 1), (3 * step, across), (3 * step, across + 1)]
    last = (3 * step, 1)
    near = [m for m in masks if m[0] < step and m != (0, 0)]
    beside = [m for m in masks if step <= m[0] < half]
    two = sorted((m for m in masks if half <= m[0] < 3 * step), key=spread)
    three = sorted((m for m in masks if m[0] >= 3 * step), key=spread)
    left = [m for m in three if m not in first + second + [last]]
    inner = two + left + [last]
    outer = two + three
    return first, second, inner, outer, near, beside


def kernel(
    row_groups, col_groups,
    table_ref, bags_ref, out_ref, pooled_ref,
    table_v, bags_v, gathered, counts, partial, arrived, halves, crossed,
    load_sem, bag_sem, own_sem, pair_sem, all_sem, send_sem, recv_sem,
    bag_send, bag_recv, sum_send, sum_recv, cross_send, cross_recv,
):
    rows, cols = row_groups, col_groups
    r, c = lax.axis_index("row"), lax.axis_index("col")
    block_len, width = table_ref.shape
    span = block_len // (rows * cols)
    own_bags, bag_len = bags_ref.shape
    per_vreg = LANES // bag_len
    half, step = rows // 2, rows // 4
    plane = lax.div(r, step)
    inner = (plane == 1) | (plane == 2)
    outer = (plane == 0) | (plane == 3)

    first, second, inner_order, outer_order, near, beside = orders(rows, cols)
    masks = [(mr, mc) for mr in range(rows) for mc in range(cols)]
    others = [m for m in masks if m != (0, 0)]
    meets = first + [(3 * step, 1), (1, 0), (0, cols // 2)]

    def peer(mask):
        return flipped(r, mask[0], rows), flipped(c, mask[1], cols)

    def at(mask):
        pr, pc = peer(mask)
        return pl.ds((pc * rows + pr) * span, span)

    def signal(sem, mask):
        pr, pc = peer(mask)
        pl.semaphore_signal(sem, inc=1, device_id=(pc, pr), device_id_type=MESH)

    def load(chosen, sem):
        for mask in chosen:
            pltpu.make_async_copy(table_ref.at[at(mask), :], table_v.at[at(mask), :], sem).start()

    def chunks(count, sem):
        whole = pl.ds(0, count * span)
        pltpu.make_async_copy(table_ref.at[whole, :], table_v.at[whole, :], sem).wait()

    def bulk(mask):
        pr, pc = peer(mask)
        return pltpu.make_async_remote_copy(
            src_ref=table_v.at[at(mask), :], dst_ref=out_ref.at[r, c],
            send_sem=send_sem, recv_sem=recv_sem,
            device_id=(pc, pr), device_id_type=MESH,
        )

    def send(chosen):
        for mask in chosen:
            bulk(mask).start()

    barrier = pltpu.get_barrier_semaphore()

    @pl.when(inner)
    def _():
        for mask in meets:
            signal(barrier, mask)

    bag_load = pltpu.make_async_copy(bags_ref, bags_v, bag_sem)
    bag_load.start()
    load(first, load_sem.at[0])
    load(second, load_sem.at[1])

    @pl.when(inner)
    def _():
        for mask in others:
            if mask[0] // step in (1, 2):
                signal(barrier, mask)

    @pl.when(outer)
    def _():
        for mask in others:
            if mask[0] // step in (0, 3):
                signal(barrier, mask)

    rest = inner_order + near + beside + [(0, 0)]
    load(rest, load_sem.at[2])
    own = pltpu.make_async_copy(table_ref.at[at((0, 0)), :], out_ref.at[r, c], own_sem)
    own.start()

    def bag(mask, kind):
        pr, _ = peer((mask, 0))
        return pltpu.make_async_remote_copy(
            src_ref=gathered.at[r], dst_ref=gathered.at[r],
            send_sem=bag_send, recv_sem=bag_recv.at[kind],
            device_id=(c, pr), device_id_type=MESH,
        )

    def pair(source):
        kind = 1
        pr, _ = peer((step, 0))
        rows_of = pl.ds(lax.div(flipped(r, source, rows), step) * step, step)
        return pltpu.make_async_remote_copy(
            src_ref=gathered.at[rows_of], dst_ref=gathered.at[rows_of],
            send_sem=bag_send, recv_sem=bag_recv.at[kind],
            device_id=(c, pr), device_id_type=MESH,
        )

    def bags(count, sem):
        whole = gathered.at[pl.ds(0, count)]
        pltpu.make_async_remote_copy(
            src_ref=whole, dst_ref=whole, send_sem=bag_send, recv_sem=sem,
            device_id=peer((1, 0))[::-1], device_id_type=MESH,
        ).wait_recv()

    bag_load.wait()
    gathered[r] = jnp.concatenate(
        [bags_v[pl.ds(q, SUBLANES, stride=per_vreg), :] for q in range(per_vreg)], axis=1
    )
    chunks(len(first), load_sem.at[0])

    @pl.when(inner)
    def _():
        pl.semaphore_wait(barrier, len(meets))
        bag(3 * step, 0).start()
        send(first)
        bag(1, 0).start()
        signal(pair_sem, (3 * step, 0))
        signal(pair_sem, (3 * step, 1))
        chunks(len(second), load_sem.at[1])
        pl.semaphore_wait(pair_sem, 2)
        bag(3 * step + 1, 0).start()
        send(second)

    tiles = block_len // LANES
    packed_rows = SUBLANES // per_vreg
    slot = (
        lax.rem(lax.broadcasted_iota(jnp.int32, (SUBLANES, LANES), 0), packed_rows) * per_vreg
        + lax.div(lax.broadcasted_iota(jnp.int32, (SUBLANES, LANES), 1), bag_len)
    )
    left_rows = lax.broadcasted_iota(jnp.int32, (tiles * SUBLANES, LANES), 0)
    right_rows = lax.broadcasted_iota(jnp.int32, (LANES, LANES), 0)

    def one_hot(numbers, first, against):
        return jnp.concatenate(
            [
                jnp.where(numbers[k:k + 1, :] == against, 1.0, 0.0).astype(jnp.bfloat16)
                for k in range(first, first + packed_rows)
            ],
            axis=1,
        )

    def enter():
        chunks(len(rest), load_sem.at[2])

        @pl.when(inner)
        def _():
            bags(half - 1, bag_recv.at[0])
            pl.semaphore_wait(all_sem, 1)
            pair(0).start()
            pair(3 * step).start()

        @pl.when(outer)
        def _():
            chunks(len(second), load_sem.at[1])
            pl.semaphore_wait(barrier, len(others))
            signal(all_sem, (step, 0))
            for mask in range(rows - 1, 0, -1):
                bag(mask, 0 if mask < step or mask >= 3 * step else 1).start()

        go(0)

    def go(n):
        @pl.when(inner)
        def _():
            send(stage(inner_order, beside, near, IN, n))

        @pl.when(outer)
        def _():
            send(stage(outer_order, beside, near, OUT, n))

    def count(turn, _):
        @pl.when(turn == 1)
        def _():
            enter()

        @pl.when((turn == 1) & outer)
        def _():
            bags(half - 1, bag_recv.at[0])

        @pl.when(turn == half)
        def _():
            bags(half, bag_recv.at[1])
            go(1)

        @pl.when(turn == half + step)
        def _():
            go(2)

        mask = turn + jnp.where(turn >= half, -step, jnp.where(turn >= step, half, 0))
        group = flipped(r, mask, rows)
        shifted = gathered[group] - r * block_len
        tile = lax.shift_right_arithmetic(shifted, LANES.bit_length() - 1)
        lane = shifted - tile * LANES
        code = tile * SUBLANES + slot
        for k in range(SUBLANES // packed_rows):
            found = lax.dot_general(
                one_hot(code, k * packed_rows, left_rows),
                one_hot(lane, k * packed_rows, right_rows),
                (((1,), (1,)), ((), ())),
                preferred_element_type=jnp.float32,
            )
            row = group * own_bags + k * SUBLANES
            for t in range(tiles):
                counts[pl.ds(row, SUBLANES), t * LANES:(t + 1) * LANES] = (
                    found[t * SUBLANES:(t + 1) * SUBLANES, :]
                )
        return 0

    lax.fori_loop(0, rows, count, 0)

    bags(rows - 1, bag_send)

    go(3)
    depth = math.gcd(block_len, 512)
    partial[...] = jnp.zeros_like(partial)

    def multiply(turn, _):
        at = pl.multiple_of(turn * depth, depth)
        block = table_v[pl.ds(at, depth), :]
        times = counts[:, pl.ds(at, depth)].astype(jnp.bfloat16)
        high = block.astype(jnp.bfloat16)
        rest = block - high.astype(jnp.float32)
        middle = rest.astype(jnp.bfloat16)
        low = (rest - middle.astype(jnp.float32)).astype(jnp.bfloat16)
        dot = functools.partial(jnp.dot, preferred_element_type=jnp.float32)
        both = dot(times, jnp.concatenate([high, middle], axis=1))
        step = (dot(times, low) + both[:, width:]) + both[:, :width]
        partial[...] += step.reshape(partial.shape)
        return 0

    lax.fori_loop(0, block_len // depth, multiply, 0)

    low, high = lax.rem(r, half), lax.div(r, half)
    for mr in range(1, half):
        pr, _ = peer((mr, 0))
        copy = pltpu.make_async_remote_copy(
            src_ref=partial.at[:, lax.rem(pr, half)], dst_ref=arrived.at[mr],
            send_sem=sum_send, recv_sem=sum_recv,
            device_id=(c, pr), device_id_type=MESH,
        )
        copy.start()

    go(4)
    for sem in (sum_send, sum_recv):
        pltpu.make_async_copy(arrived.at[pl.ds(1, half - 1)], arrived.at[pl.ds(1, half - 1)], sem).wait()
    total = partial[:, low]
    for mr in range(1, half):
        total += arrived[mr]
    halves[...] = total
    own.wait()
    other, _ = peer((half, 0))
    across = pltpu.make_async_remote_copy(
        src_ref=halves.at[1 - high], dst_ref=crossed,
        send_sem=cross_send, recv_sem=cross_recv,
        device_id=(c, other), device_id_type=MESH,
    )
    across.start()

    go(5)
    across.wait()
    go(6)
    pooled_ref[...] = halves[high] + crossed[...]
    moved = pl.ds(0, len(others) * span)
    for sem in (send_sem, recv_sem):
        pltpu.make_async_copy(table_ref.at[moved, :], table_v.at[moved, :], sem).wait()


def stage(far, beside, near, cuts, n):
    def part(chosen, ends):
        ends = (0,) + ends + (len(chosen),)
        return chosen[ends[n]:ends[n + 1]]

    one, two, three = part(far, cuts[0]), part(beside, cuts[1]), part(near, cuts[2])
    result = []
    for k in range(max(len(one), len(two))):
        result += two[k:k + 1] + one[k:k + 1]
    return result + three


IN = (5, 5, 5, 5, 5, 11), (0, 0, 0, 0, 8, 8), (0, 0, 0, 0, 0, 7)
OUT = (0, 0, 0, 0, 4, 16), (2, 2, 2, 2, 4, 8), (3, 3, 3, 3, 7, 7)


def per_device(column_table, bag_rows):
    rows, cols = lax.axis_size("row"), lax.axis_size("col")
    block_len, width = column_table.shape
    own_bags, bag_len = bag_rows.shape
    span = block_len // (rows * cols)
    fits = (
        width % LANES == 0 and LANES % bag_len == 0 and bag_len * SUBLANES >= LANES and own_bags * bag_len == SUBLANES * LANES
        and span % SUBLANES == 0 and block_len % LANES == 0
        and rows // 4 == 2 and rows % 4 == 0 and cols >= 4 and cols & (cols - 1) == 0
    )
    if not fits:
        return general(column_table, bag_rows)
    bags = own_bags * rows
    half = rows // 2
    dma = pltpu.SemaphoreType.DMA
    landed, sums = pl.pallas_call(
        functools.partial(kernel, rows, cols),
        out_shape=(
            jax.ShapeDtypeStruct((rows, cols, span, width), jnp.float32),
            jax.ShapeDtypeStruct((own_bags, width), jnp.float32),
        ),
        in_specs=[pl.BlockSpec(memory_space=pltpu.HBM), pl.BlockSpec(memory_space=pltpu.HBM)],
        out_specs=(pl.BlockSpec(memory_space=pltpu.VMEM), pl.BlockSpec(memory_space=pltpu.VMEM)),
        scratch_shapes=[
            pltpu.VMEM((block_len, width), jnp.float32),
            pltpu.VMEM((own_bags, bag_len), jnp.int32),
            pltpu.VMEM((rows, SUBLANES, LANES), jnp.int32),
            pltpu.VMEM((bags, block_len), jnp.float32),
            pltpu.VMEM((2, half, own_bags, width), jnp.float32),
            pltpu.VMEM((half, 2, own_bags, width), jnp.float32),
            pltpu.VMEM((2, own_bags, width), jnp.float32),
            pltpu.VMEM((own_bags, width), jnp.float32),
            dma((3,)), dma, dma,
            pltpu.SemaphoreType.REGULAR, pltpu.SemaphoreType.REGULAR,
            dma, dma,
            dma, dma((2,)), dma, dma, dma, dma,
        ],
        compiler_params=pltpu.CompilerParams(
            collective_id=0, has_side_effects=True, vmem_limit_bytes=32 * 1024 * 1024
        ),
    )(
        pltpu.with_memory_space_constraint(column_table, pltpu.HBM),
        pltpu.with_memory_space_constraint(bag_rows, pltpu.HBM),
    )
    return pl.pallas_call(
        write_out,
        out_shape=(
            jax.ShapeDtypeStruct((rows, span, width * cols), jnp.float32),
            jax.ShapeDtypeStruct((own_bags, width), jnp.float32),
        ),
        in_specs=[pl.BlockSpec(memory_space=pltpu.VMEM)] * 2,
        out_specs=(pl.BlockSpec(memory_space=pltpu.HBM), pl.BlockSpec(memory_space=pltpu.HBM)),
        scratch_shapes=[dma, dma],
        compiler_params=pltpu.CompilerParams(vmem_limit_bytes=8 * 1024 * 1024),
    )(landed, sums)


def write_out(landed_ref, sums_ref, out_ref, pooled_ref, sem, sum_sem):
    cols, width = landed_ref.shape[1], landed_ref.shape[3]
    for c in range(cols):
        pltpu.make_async_copy(
            landed_ref.at[:, c], out_ref.at[:, :, c * width:(c + 1) * width], sem
        ).start()
    pooled = pltpu.make_async_copy(sums_ref, pooled_ref, sum_sem)
    pooled.start()
    pooled.wait()
    pltpu.make_async_copy(out_ref, out_ref, sem).wait()


def solution(mesh):
    return jax.shard_map(
        per_device,
        mesh=mesh,
        in_specs=(P("row", "col"), P("row", None)),
        out_specs=(P(None, ("col", "row"), None), P("row", "col")),
        check_vma=False,
    )
```
